8 devices in a mesh: dp: 2 (over y, z), tp: 4 (over x, core).
Axes of the slice: x: 2, y: 2, z: 1, core: 2. Of those that a mesh axis runs over, the one named last changes fastest.
Arguments:
- x: bfloat16 [2, 1536, 3584], P('dp', 'tp'), parts along dimension 0
- dy: bfloat16 [2, 1536, 3584], P('dp', 'tp'), parts along dimension 0
- wq: bfloat16 [3584, 4096], P(None, 'tp')
- wk: bfloat16 [3584, 2048], P(None, 'tp')
- wv: bfloat16 [3584, 2048], P(None, 'tp')
- wo: bfloat16 [4096, 3584], P('tp')
- w_gate: bfloat16 [3584, 14336], P(None, 'tp')
- w_up: bfloat16 [3584, 14336], P(None, 'tp')
- w_down: bfloat16 [14336, 3584], P('tp')
Outputs:
- output 1: bfloat16 [2, 1536, 3584], P('dp', 'tp'), parts along dimension 0
- output 2: bfloat16 [7168, 4096], P('dp', 'tp'), parts along dimension 0
- output 3: bfloat16 [7168, 2048], P('dp', 'tp'), parts along dimension 0
- output 4: bfloat16 [7168, 2048], P('dp', 'tp'), parts along dimension 0
- output 5: bfloat16 [8192, 3584], P(('dp', 'tp')), parts along dimension 0
- output 6: bfloat16 [7168, 14336], P('dp', 'tp'), parts along dimension 0
- output 7: bfloat16 [7168, 14336], P('dp', 'tp'), parts along dimension 0
- output 8: bfloat16 [28672, 3584], P(('dp', 'tp')), parts along dimension 0
There are 2 independent parts. The reference program is written for one: setup_inputs(seed, part) draws one part's arguments, and reference() takes and returns one part's arrays. A program takes and returns all parts, laid end to end along the dimension named above; an argument that names none is the same for every part.
All inputs are finite; a program needn't handle non-finite values.
Results may differ from the reference program's by a relative error of at most 0.024.
Values are sent between devices in bfloat16 or wider.
A program may use at most 2 GiB of HBM per device.

```python
import jax
import jax.numpy as jnp
from jax import lax

SEQUENCES = 1
TOKENS = 1536
D = 3584
HEADS = 16
KV_HEADS = 8
HEAD = 256
FF = 14336
THETA = 10000
NAMES = ("wq", "wk", "wv", "wo", "w_gate", "w_up", "w_down")
SHAPES = {
    "wq": (D, HEADS * HEAD),
    "wk": (D, KV_HEADS * HEAD),
    "wv": (D, KV_HEADS * HEAD),
    "wo": (HEADS * HEAD, D),
    "w_gate": (D, FF),
    "w_up": (D, FF),
    "w_down": (FF, D),
}


def bump(key, n, height):
    away = (jnp.arange(n, dtype=jnp.int32) - jax.random.randint(key, (), 0, n, jnp.int32)) % n
    return jnp.where(away < n // 8, height, 1.0)


def together(key, own, strength):
    shared = jax.random.normal(key, own.shape[1:], jnp.float32)
    return (own + strength * shared) * lax.rsqrt(1 + strength * strength)


def setup_inputs(seed: int = 0, part: int = 0) -> dict:
    kx, kdy, ka, kb, kz, kf, kh, kl, *kw = jax.random.split(jax.random.key(seed), 8 + len(NAMES))
    kx, kdy, ka, kb = (jax.random.fold_in(k, part) for k in (kx, kdy, ka, kb))
    shape = (SEQUENCES, TOKENS, D)
    much_x, much_dy = jax.random.uniform(kz, (2,), jnp.float32, 0.0, 1.0)
    loud = 2.0 ** jax.random.uniform(jax.random.fold_in(kz, 1), (), jnp.float32, -1.0, 2.0)
    halves = 2.0 ** jax.random.uniform(kl, (2,), jnp.float32, -1.0, 1.0)
    times = {"wq": 1.0, "wk": 1.0, "wv": 2.0, "wo": halves[0], "w_gate": 1.0, "w_up": bump(kh, FF, 4.0), "w_down": halves[1]}
    x = together(ka, jax.random.normal(kx, shape, jnp.float32), much_x) * bump(kf, D, 4.0)
    dy = together(kb, jax.random.normal(kdy, shape, jnp.float32), much_dy)
    drawn = {"x": x.astype(jnp.bfloat16), "dy": (loud * dy * (SEQUENCES * TOKENS) ** -0.5).astype(jnp.bfloat16)}
    for key, name in zip(kw, NAMES, strict=True):
        drawn[name] = (jax.random.normal(key, SHAPES[name], jnp.float32) * SHAPES[name][0] ** -0.5 * times[name]).astype(jnp.bfloat16)
    return drawn


def matmul(a, w):
    return jnp.dot(a, w, preferred_element_type=jnp.float32).astype(jnp.bfloat16)


def normed(h):
    wide = h.astype(jnp.float32)
    scale = lax.rsqrt(jnp.mean(wide**2, -1, keepdims=True) + 1e-6)
    return (wide * scale).astype(jnp.bfloat16)


def turned(t, theta):
    half = t.shape[-1] // 2
    angle = jnp.arange(t.shape[0], dtype=jnp.float32)[:, None] * theta ** (-jnp.arange(half, dtype=jnp.float32) / half)
    cos, sin = jnp.cos(angle)[:, None], jnp.sin(angle)[:, None]
    a, b = t[..., :half].astype(jnp.float32), t[..., half:].astype(jnp.float32)
    return jnp.concatenate([a * cos - b * sin, b * cos + a * sin], -1).astype(jnp.bfloat16)


def seen_by(q, k, v):
    tokens, kv = q.shape[0], k.shape[1]
    q = q.reshape(tokens, kv, -1, q.shape[-1])
    scores = jnp.einsum("tgsd,ugd->gstu", q.astype(jnp.float32), k.astype(jnp.float32)) * q.shape[-1] ** -0.5
    place = jnp.arange(tokens)
    weights = jax.nn.softmax(jnp.where(place[:, None] >= place, scores, -jnp.inf), -1).astype(jnp.bfloat16)
    return jnp.einsum("gstu,ugd->tgsd", weights.astype(jnp.float32), v.astype(jnp.float32)).astype(jnp.bfloat16).reshape(tokens, -1)


def layer(h, w):
    a = normed(h)
    q, k = (turned(matmul(a, w[name]).reshape(h.shape[0], -1, HEAD), THETA) for name in ("wq", "wk"))
    h = h + matmul(seen_by(q, k, matmul(a, w["wv"]).reshape(h.shape[0], -1, HEAD)), w["wo"])
    b = normed(h)
    gate = jnp.dot(b, w["w_gate"], preferred_element_type=jnp.float32)
    up = jnp.dot(b, w["w_up"], preferred_element_type=jnp.float32)
    return h + matmul((jax.nn.silu(gate) * up).astype(jnp.bfloat16), w["w_down"])


def reference(x, dy, wq, wk, wv, wo, w_gate, w_up, w_down):
    weights = dict(zip(NAMES, (wq, wk, wv, wo, w_gate, w_up, w_down), strict=True))

    def take(so_far, sequence):
        h, by_y = sequence
        _, back = jax.vjp(lambda w, h: layer(h, w), weights, h)
        by_weights, by_h = back(by_y)
        return jax.tree.map(lambda total, term: total + term.astype(jnp.float32), so_far, by_weights), by_h

    none_yet = {name: jnp.zeros(w.shape, jnp.float32) for name, w in weights.items()}
    by_weights, by_x = lax.scan(take, none_yet, (x, dy))
    return (by_x, *(by_weights[name].astype(jnp.bfloat16) for name in NAMES))
```

```python
import functools

import jax
import jax.numpy as jnp
from jax import lax
from jax.experimental import pallas as pl
from jax.experimental.pallas import tpu as pltpu
from jax.sharding import PartitionSpec as P


LOG2E = 1.4426950408889634
NEG = -1e30
HIDDEN = 2 * NEG
VMEM = 60 * 2**20
HEAD = 256
HALF = HEAD // 2
QW, KV = 1024, 512
TILE, WIDE = 896, 1792
THETA = 10000
CORE = [(0, 1), (1, 0), (2, 3), (3, 2)]
CHIP = [(0, 2), (2, 0), (1, 3), (3, 1)]
BF = jnp.bfloat16
F32 = jnp.float32


def _fit(size, want, unit=128):
    return max(n for n in range(unit, max(min(want, size), unit) + 1, unit) if size % n == 0)


def nn(a, b):
    return lax.dot_general(a, b, (((1,), (0,)), ((), ())), preferred_element_type=F32)


def nt(a, b):
    return lax.dot_general(a, b, (((1,), (1,)), ((), ())), preferred_element_type=F32)


def tn(a, b):
    return lax.dot_general(a, b, (((0,), (0,)), ((), ())), preferred_element_type=F32)


def rows(refs):
    got = [r[:] for r in refs]
    return got[0] if len(got) == 1 else jnp.concatenate(got, axis=0)


def hbm(array):
    return array, None, None


def call(body, me, grid, ins, outs, flops, scratch=(), aliases=None, vmem=VMEM):
    specs = [pl.BlockSpec(memory_space=pl.ANY) if block is None else pl.BlockSpec(block, at, **dict.fromkeys(["pipeline_mode"] * len(more), pl.Buffered(1)))
             for _, block, at, *more in ins]
    arrays = [a for a, *_ in ins]
    moved = sum(a.size * a.dtype.itemsize for a in arrays)
    got = pl.pallas_call(
        body,
        grid_spec=pltpu.PrefetchScalarGridSpec(
            num_scalar_prefetch=1, grid=grid, in_specs=specs,
            out_specs=[pl.BlockSpec(block, at) for _, _, block, at in outs], scratch_shapes=list(scratch)),
        out_shape=[jax.ShapeDtypeStruct(shape, dtype) for shape, dtype, _, _ in outs],
        input_output_aliases={} if aliases is None else aliases,
        compiler_params=pltpu.CompilerParams(dimension_semantics=("arbitrary",) * len(grid), vmem_limit_bytes=vmem),
        cost_estimate=pl.CostEstimate(flops=int(flops), bytes_accessed=moved, transcendentals=0),
    )(me, *arrays)
    return got


ROWS = 24 * 2**20
STEP = 96
STRIP = 16


def strips(work, *refs):
    for at in range(0, STEP, STRIP):
        work(*(ref.at[at : at + STRIP] for ref in refs))


def wide(ref):
    return ref[:].astype(F32)


def by_rows(shift=0):
    return lambda i, me: (i + shift, 0)


def row_kernel(body, me, ins, outs, steps, vmem=VMEM, into=None):
    d = ins[0][0].shape[1]
    specs = [(a, (STEP, d), by_rows(first)) for a, first in ins]
    aliases = {}
    if into is not None:
        aliases = {1 + len(specs): 0}
        specs.append(hbm(into))
    return call(body, me, (steps,), specs, [((n, d), BF, (STEP, d), by_rows(first)) for n, first in outs], 9 * steps * STEP * d, aliases=aliases, vmem=vmem)


def _normed(wide):
    return (wide * lax.rsqrt(jnp.mean(wide * wide, -1, keepdims=True) + 1e-6)).astype(BF)


def _norm(me, x_ref, *a_refs, per):
    for n, ref in enumerate(a_refs):
        @pl.when(pl.program_id(0) // per == n)
        def _():
            ref[:] = _normed(wide(x_ref))


def _halves(body, me, ins, d):
    n = ins[0].shape[0]
    per = n // 2 // STEP
    outs = [((n // 2, d), BF, (STEP, d), lambda i, me: (jnp.minimum(i, per - 1), 0)), ((n // 2, d), BF, (STEP, d), lambda i, me: (jnp.maximum(i - per, 0), 0))]
    return call(functools.partial(body, per=per), me, (2 * per,), [(t, (STEP, d), by_rows()) for t in ins], outs, 4 * n * d, vmem=ROWS)


def norm(me, x):
    return _halves(_norm, me, [x], x.shape[1])


def _add(me, a_ref, b_ref, *o_refs, per):
    for n, ref in enumerate(o_refs):
        @pl.when(pl.program_id(0) // per == n)
        def _():
            ref[:] = (wide(a_ref) + wide(b_ref)).astype(BF)


def add(me, a, b):
    n = a.shape[0]
    return row_kernel(functools.partial(_add, per=n), me, [(a, 0), (b, 0)], [(n, 0)], n // STEP)[0]


def add_halves(me, a, b):
    return _halves(_add, me, [a, b], a.shape[1])


def _join(me, p_ref, c_ref, r_ref, x_ref, *refs):
    def work(p, c, r, x, h_ref, b_ref):
        h = (wide(x) + (wide(p) + wide(c) + wide(r)).astype(BF).astype(F32)).astype(BF)
        h_ref[:] = h
        b_ref[:] = _normed(h.astype(F32))

    strips(work, p_ref, c_ref, r_ref, x_ref, *refs[-2:])


def join(me, half, p, c, r, x, into=None):
    n = x.shape[0]
    per = n // 2 // STEP
    return row_kernel(_join, me, [(p, half * per), (c, half * per), (r, 0), (x, half * per)], [(n, half * per), (n // 2, 0)], per, into=into)


def _unjoin(me, *refs):
    def work(p, c, r, h_ref, g, o_ref):
        by = (wide(p) + wide(c) + wide(r)).astype(BF).astype(F32)
        h = wide(h_ref)
        scale = lax.rsqrt(jnp.mean(h * h, -1, keepdims=True) + 1e-6)
        mix = jnp.sum(by * h, -1, keepdims=True) * (scale * scale * scale / h.shape[1])
        o_ref[:] = (wide(g) + (by * scale - h * mix).astype(BF).astype(F32)).astype(BF)

    strips(work, *refs)


def unjoin(me, p, c, r, h, g):
    n = h.shape[0]
    return row_kernel(_unjoin, me, [(t, 0) for t in (p, c, r, h, g)], [(n, 0)], n // STEP)[0]


def turn(t, cos, sin):
    got = []
    for at in range(0, t.shape[1], HEAD):
        a, b = t[:, at : at + HALF], t[:, at + HALF : at + HEAD]
        got += [a * cos - b * sin, b * cos + a * sin]
    return jnp.concatenate(got, axis=1).astype(BF)


CHUNKS = 2


def copy(src, dst, sem):
    return pltpu.make_async_copy(src, dst, sem)


def _matmul(me, *refs, chunks, left, right, sides, pairs, form, steps, block, source, put, outs):
    refs = list(refs)

    def take(count):
        got, refs[:] = refs[:count], refs[count:]
        return got

    a_refs = [take(len(pieces)) for pieces in left]
    w_refs, x_refs = take(len(right)), take(len(sides))
    refs[:] = refs[len(refs) - outs - 2 * len(left) - 3 * len(source) - 2 * len(sides) :]
    o_refs = take(outs)
    a_s, a_sem, w_s, w_sem, first_sem, x_s, x_sem = take(len(left)), take(len(left)), take(len(source)), take(len(source)), take(len(source)), take(len(sides)), take(len(sides))
    j = pl.program_id(0)
    slot = lax.rem(j, 2)

    def part(c, size):
        return pl.ds(c * (size // chunks), size // chunks)

    def a_copies(c):
        for pieces, ins, dst, sems in zip(left, a_refs, a_s, a_sem):
            at = 0
            for p, ((size, where, col, k), ref) in enumerate(zip(pieces, ins)):
                first = where(me) * size
                cols = pl.ds(col * k + c * (k // chunks), k // chunks)
                yield copy(ref.at[pl.ds(pl.multiple_of(first, size), size), cols], dst.at[pl.ds(at, size), part(c, k)], sems.at[p, c])
                at += size

    def w_first(c):
        for pick, dst, sems in zip(source, w_s, first_sem):
            ref, at = pick(w_refs, 0)
            k = dst.shape[1 if form is nn else 2]
            src = ref.at[part(c, k), pl.ds(at, block)] if form is nn else ref.at[pl.ds(at, block), part(c, k)]
            yield copy(src, dst.at[0, part(c, k), :] if form is nn else dst.at[0, :, part(c, k)], sems.at[c])

    def w_copies(step, at_slot):
        for pick, dst, sems in zip(source, w_s, w_sem):
            ref, at = pick(w_refs, step)
            yield copy(ref.at[:, pl.ds(at, block)] if form is nn else ref.at[pl.ds(at, block), :], dst.at[at_slot], sems.at[at_slot])

    def x_copies(step, at_slot):
        for (per_step, where), ref, dst, sem in zip(sides, x_refs, x_s, x_sem):
            if per_step:
                yield copy(ref.at[:, pl.ds(step * block, block)], dst.at[at_slot], sem.at[at_slot])
            elif isinstance(step, int) and step == 0:
                yield copy(ref.at[pl.ds(where(me), dst.shape[0]), :], dst, sem)

    def begin(step, at_slot):
        for each in (*w_copies(step, at_slot), *x_copies(step, at_slot)):
            each.start()

    def ahead():
        if isinstance(source[0](w_refs, 0)[1], int) and len(right) > len(source):
            for step in range(2, steps):
                pl.when(j == step - 1)(functools.partial(begin, step, step % 2))
        else:
            pl.when(j + 1 < steps)(lambda: begin(j + 1, 1 - slot))

    def finish(totals, at_slot):
        put(me, j, totals, [x.at[at_slot] if side[0] else x for side, x in zip(sides, x_s)], o_refs)

    @pl.when(j == 0)
    def _():
        for c in range(chunks):
            for each in (*a_copies(c), *w_first(c)):
                each.start()
        for each in x_copies(0, 0):
            each.start()
        if steps > 1:
            begin(1, 1)
        totals = {}
        for c in range(chunks):
            for each in (*a_copies(c), *w_first(c)):
                each.wait()
            for l, r, t in pairs:
                k = a_s[l].shape[1]
                w = w_s[r][0, part(c, k), :] if form is nn else w_s[r][0, :, part(c, k)]
                got = form(a_s[l][:, part(c, k)], w)
                totals[t] = totals[t] + got if t in totals else got
        for each in x_copies(0, 0):
            each.wait()
        finish(totals, 0)

    @pl.when(j > 0)
    def _():
        ahead()
        for each in (*w_copies(1, slot), *x_copies(1, slot)):
            each.wait()
        totals = {}
        for l, r, t in pairs:
            got = form(a_s[l][:], w_s[r][slot])
            totals[t] = totals[t] + got if t in totals else got
        finish(totals, slot)


by_step = lambda r, block: lambda refs, step: (refs[r], step * block)


def matmul(me, left, right, pairs, form, block, steps, put, outs, sides=(), source=None, into=(), chunks=CHUNKS):
    rows_of = [sum(p[1] for p in pieces) for pieces in left]
    source = [by_step(r, block) for r in range(len(right))] if source is None else source
    ks = [right[r].shape[form is nt] for r in range(len(source))]
    ins = [(p[0], None, None) for pieces in left for p in pieces] + [(w, None, None) for w in right] + [(x[0], None, None) for x in sides]
    aliases = {1 + len(ins) + i: i for i in range(len(into))}
    ins += [(t, None, None) for t in into]
    dma = pltpu.SemaphoreType.DMA
    scratch = [pltpu.VMEM((m, pieces[0][4]), BF) for m, pieces in zip(rows_of, left)] + [dma((len(pieces), chunks)) for pieces in left]
    scratch += [pltpu.VMEM((2, k, block) if form is nn else (2, block, k), BF) for k in ks] + [dma((2,)) for _ in ks] + [dma((chunks,)) for _ in ks]
    scratch += [pltpu.VMEM((2, x[0].shape[0], block) if x[1] else (x[2][1], x[0].shape[1]), x[0].dtype) for x in sides] + [dma((2,)) if x[1] else dma for x in sides]
    body = functools.partial(_matmul, chunks=chunks, left=[[(p[1], p[2], p[3], p[4]) for p in pieces] for pieces in left], right=right, pairs=pairs, form=form, steps=steps,
                             sides=[(x[1], None if x[1] else x[2][0]) for x in sides], block=block, source=source, put=put, outs=len(outs))
    flops = 2 * steps * block * sum(rows_of[l] * ks[r] for l, r, _ in pairs)
    return call(body, me, (steps,), ins, outs, flops, scratch, aliases)


def _put_qkv(me, j, totals, sides, o_refs, *, half, tops):
    got = totals[0].astype(BF)
    cos_ref, sin_ref = sides
    for i, top in enumerate(tops):
        at = pl.multiple_of(top(me), half)
        part = got[i * half : (i + 1) * half]
        turned = turn(part.astype(F32), cos_ref[pl.ds(at, half), :], sin_ref[pl.ds(at, half), :])
        o_refs[0][pl.ds(at, half), :] = jnp.where(j < 3, turned, part)


def qkv(me, parts, slots, w, cos, sin, into=()):
    half = sum(a.shape[0] for a in parts) // 2
    chip = lambda me: (me[0] ^ slots[0]) // 2
    tops = [functools.partial(lambda me, s: (me[0] ^ s) % 2 * half, s=s) for s in slots]
    pick = lambda refs, step: (refs[max(step - 1, 0)], 512 if step == 1 else 0)
    side = lambda t: (t, False, (lambda me: pl.multiple_of(chip(me) * 2 * half, 2 * half), 2 * half))
    return matmul(me, [[piece(a, a.shape[0]) for a in parts]], [w["wq"], w["wk"], w["wv"]], [(0, 0, 0)], nn, KV, 4,
                  functools.partial(_put_qkv, half=half, tops=tops), [((4 * half, 2048), BF, (2 * half, KV), lambda j, me: (chip(me), j))],
                  [side(cos), side(sin)], [pick], into)[0]


def _put_terms(me, j, totals, sides, o_refs):
    total, at = totals[0].astype(BF), 0
    for o_ref in o_refs:
        o_ref[:] = total[at : at + o_ref.shape[0]]
        at += o_ref.shape[0]


def terms(me, pairs, form, block, joined=False, chunks=CHUNKS):
    cols = pairs[0][1].shape[form is nn]
    sizes = [p[1] for p in pairs[0][0]]
    outs = [((size, cols), BF, (size, block), lambda j, me: (0, j)) for size in ([sum(sizes)] if joined else sizes)]
    return matmul(me, [p[0] for p in pairs], [p[1] for p in pairs], [(i, i, 0) for i in range(len(pairs))], form, block, cols // block, _put_terms, outs, chunks=chunks)


def _put_hidden(me, j, totals, sides, o_refs):
    gate, up, by = totals[0], totals[1], sides[0][:].astype(F32)
    sig = 1 / (1 + jnp.exp(-gate))
    silu = gate * sig
    hid_ref, dg_ref, du_ref = o_refs
    hid_ref[:] = (silu * up).astype(BF)
    du_ref[:] = (by * silu).astype(BF)
    dg_ref[:] = (by * up * (sig * (1 + gate * (1 - sig)))).astype(BF)


def hidden(me, parts, w_gate, w_up, by, block, place, into=()):
    f, m = w_gate.shape[1], by.shape[0]
    outs = [((2 * m, f), BF, (m, block), lambda j, me: (place, j))] * 3
    return matmul(me, [[piece(p, p.shape[0]) for p in parts]], [w_gate, w_up], [(0, 0, 0), (0, 1, 1)], nn, block,
                  f // block, _put_hidden, outs, [(by, True, None)], None, into)


def _outer(me, *refs, na, nb):
    refs[-1][:] = tn(rows(refs[:na]), rows(refs[na : na + nb])).astype(BF)


def piece(array, size, where=None, col=0, k=None):
    return (array, size, (lambda me: 0) if where is None else where, col, array.shape[1] if k is None else k)


def outer(me, left, right, bm, bn, span=None, into=None):
    ins, tokens = [], sum(p[1] for p in left)
    m, n = left[0][4], right[0][4]
    first, last = (0, m // bm) if span is None else span
    for pieces, block, axis in ((left, bm, 0), (right, bn, 1)):
        for array, size, where, col, k in pieces:
            at = functools.partial(lambda i, j, me, where, axis, shift: (where(me), (i, j)[axis] + shift), where=where, axis=axis,
                                   shift=col * (k // block) + first * (1 - axis))
            ins.append((array, (size, block), at))
    if into is not None:
        ins.append(hbm(into))
    return call(functools.partial(_outer, na=len(left), nb=len(right)), me, (last - first, n // bn), ins,
                [((m, n), BF, (bm, bn), lambda i, j, me: (i + first, j))], 2 * tokens * (last - first) * bm * n,
                aliases=None if into is None else {len(ins): 0})[0]


def _outer_qkv(me, *refs, n, m):
    j = pl.program_id(1)
    got = tn(rows(refs[:n]), jnp.where(j == 0, rows(refs[n : n + m]), rows(refs[n + m : n + 2 * m]))).astype(BF)
    q_ref, k_ref, v_ref = refs[-3:]

    @pl.when(j == 0)
    def _():
        q_ref[:] = got

    @pl.when(j > 0)
    def _():
        k_ref[:], v_ref[:] = got[:, :KV], got[:, KV:]


def outer_qkv(me, left, dq, dkv, slots, bm):
    d, n = left[0][0].shape[1], dq.shape[0] // len(slots)
    ins = [(a, (size, bm), lambda i, j, me: (0, i)) for a, size, *_ in left]
    ins += [(t, (n, QW), functools.partial(lambda i, j, me, s: (me[0] ^ s, 0), s=s)) for t in (dq, dkv) for s in slots]
    outs = [((d, width), BF, (bm, width), lambda i, j, me: (i, 0)) for width in (QW, KV, KV)]
    return call(functools.partial(_outer_qkv, n=len(left), m=len(slots)), me, (d // bm, 2), ins, outs, 2 * dq.shape[0] * d * 2048)


def _put_heads(me, j, totals, sides, o_refs, *, size):
    got = totals[0].astype(BF)
    for s in range(got.shape[0] // size):
        o_refs[0][pl.ds(pl.multiple_of((me[0] ^ s) * size, size), size), :] = got[s * size : (s + 1) * size]


def heads_by(me, parts, wo, block):
    size = parts[0].shape[0]
    outs = [((4 * size, wo.shape[0]), BF, (4 * size, block), lambda j, me: (0, j))]
    return matmul(me, [[piece(p, size) for p in parts]], [wo], [(0, 0, 0)], nt, block, wo.shape[0] // block,
                  functools.partial(_put_heads, size=size), outs)[0]


def q_cols(h):
    return slice(h * HEAD, h * HEAD + HEAD)


def k_cols(h):
    return q_cols(h // 2)


def v_cols(h):
    return q_cols(h // 2 + 2)


def _gap(bk, wide):
    return lax.broadcasted_iota(jnp.int32, (bk, wide), 1) - lax.broadcasted_iota(jnp.int32, (bk, wide), 0)


def _attend(me, q_ref, kv_ref, wo_ref, *rest, slots, n, wide):
    *p_refs, o_ref, lse_ref, top_s, mix_s, gap_s = rest[-5 - len(slots) :]
    i = pl.program_id(0)
    mine = me[0] ^ (slots[0] - i)
    scale = HEAD**-0.5
    e = scale * LOG2E
    heads = q_ref.shape[1] // HEAD
    pieces = [(h, at) for h in range(heads) for at in range(0, n, wide)]

    @pl.when(i == 0)
    def _():
        gap_s[:] = _gap(n, wide)

    top_s[:] = jnp.full_like(top_s, NEG)
    mix_s[:] = jnp.zeros_like(mix_s)
    ones = jnp.ones((8, n), BF)

    def block(j, masked):
        here = pl.ds(pl.multiple_of(j * n, n), n)
        scores = [nt(kv_ref[here, k_cols(h)], q_ref[at : at + wide, q_cols(h)]) for h, at in pieces]
        weights, keeps = [], []
        for (h, at), s in zip(pieces, scores):
            if masked:
                s = jnp.where(gap_s[:] >= -at, s, HIDDEN)
            old = top_s[h : h + 1, at : at + wide]
            top = jnp.maximum(old, s.max(axis=0, keepdims=True))
            top_s[h : h + 1, at : at + wide] = top
            weights.append(jnp.exp2((s - top) * e).astype(BF))
            keeps.append(jnp.exp2((old - top) * e))
        for (h, at), p, keep in zip(pieces, weights, keeps):
            v = kv_ref[here, v_cols(h)]
            values = jnp.concatenate([v.T, ones], axis=0)
            mix_s[h, :, at : at + wide] = mix_s[h, :, at : at + wide] * keep + nn(values, p)

    lax.fori_loop(0, mine, lambda j, _: block(j, False), None)
    block(mine, True)
    for h in range(heads):
        top, total = top_s[h : h + 1, :], mix_s[h, HEAD : HEAD + 1, :]
        o_ref[:, q_cols(h)] = (mix_s[h, :HEAD, :] * (1 / total)).T.astype(BF)
        lse_ref[h : h + 1, :] = top * scale + jnp.log(total)
    for k, p_ref in enumerate(p_refs):
        @pl.when(i == k)
        def _():
            for at in range(0, p_ref.shape[1], 896):
                p_ref[:, at : at + 896] = nn(o_ref[:], wo_ref[:, at : at + 896]).astype(BF)


def attend(me, qkv, wo, slots, into=()):
    t, d = qkv.shape[0], wo.shape[1]
    n = t // 4
    wide = _fit(n, KV)
    mine = lambda i, me: me[0] ^ (slots[0] - i)
    ins = [(qkv, (n, QW), lambda i, me: (mine(i, me), 0)), (qkv, (t, QW), lambda i, me: (0, 1), 1), (wo, wo.shape, lambda i, me: (0, 0), 1)]
    aliases = {1 + len(ins) + i: len(slots) + i for i in range(len(into))}
    ins += [(a, None, None) for a in into]
    outs = [((n, d), BF, (n, d), lambda i, me: (0, 0))] * len(slots)
    outs += [((t, QW), BF, (n, QW), lambda i, me: (mine(i, me), 0)), ((4, t), F32, (4, n), lambda i, me: (0, mine(i, me)))]
    return call(functools.partial(_attend, slots=slots, n=n, wide=wide), me, (len(slots),), ins, outs, 2 * 2 * n * (4 * 512 * t // 2 + QW * d),
                [pltpu.VMEM((8, n), F32), pltpu.VMEM((4, HEAD + 8, n), F32), pltpu.VMEM((n, wide), jnp.int32)], aliases)


def _attend_by(me, q_ref, kv_ref, do_ref, o_ref, lse_ref, cos_ref, sin_ref, dq_ref, dkv_ref, dq_s, dkv_s, gap_s, *, bq, bk, wide):
    iq = pl.program_id(0)
    scale = HEAD**-0.5
    e = scale * LOG2E
    heads = q_ref.shape[1] // HEAD
    pieces = [(h, at) for h in range(heads) for at in range(0, bq, wide)]

    @pl.when(iq == 0)
    def _():
        gap_s[:] = _gap(bk, wide)
        dkv_s[:] = jnp.zeros_like(dkv_s)

    dq_s[:] = jnp.zeros_like(dq_s)
    lses = [lse_ref[h : h + 1, at : at + wide] * LOG2E for h, at in pieces]
    deltas = []
    for h, at in pieces:
        own = (slice(at, at + wide), q_cols(h))
        deltas.append((do_ref[own].astype(F32) * o_ref[own].astype(F32)).T.sum(axis=0, keepdims=True))

    def block(j, masked):
        here = pl.ds(pl.multiple_of(j * bk, bk), bk)
        k_of = lambda h: kv_ref[here, k_cols(h)]
        v_of = lambda h: kv_ref[here, v_cols(h)]
        qs = [q_ref[at : at + wide, q_cols(h)] for h, at in pieces]
        dos = [do_ref[at : at + wide, q_cols(h)] for h, at in pieces]
        scores = [nt(k_of(h), x) for (h, _), x in zip(pieces, qs)]
        dps = [nt(v_of(h), x) for (h, _), x in zip(pieces, dos)]
        for n, (h, at) in enumerate(pieces):
            p = jnp.exp2(scores[n] * e - lses[n])
            if masked:
                p = jnp.where(gap_s[:] >= j * bk - iq * bq - at, p, 0.0)
            ds = (p * (dps[n] - deltas[n])).astype(BF)
            dkv_s[here, v_cols(h)] += nn(p.astype(BF), dos[n])
            dkv_s[here, k_cols(h)] += nn(ds, qs[n])
            dq_s[h, :, at : at + wide] += nn(k_of(h).T, ds)

    lax.fori_loop(0, iq * bq // bk, lambda j, _: block(j, False), None)
    lax.fori_loop(iq * bq // bk, ((iq + 1) * bq + bk - 1) // bk, lambda j, _: block(j, True), None)
    mine = pl.ds(pl.multiple_of(iq * bq, bq), bq)
    cos, sin = cos_ref[mine, :], sin_ref[mine, :]
    for h in range(heads):
        dq = (dq_s[h] * scale).T.astype(BF).astype(F32)
        dq_ref[:, q_cols(h)] = turn(dq, cos, -sin)

    @pl.when(iq == pl.num_programs(0) - 1)
    def _():
        dk = (dkv_s[:, :KV] * scale).astype(BF).astype(F32)
        dkv_ref[:, :KV] = turn(dk, cos_ref[:], -sin_ref[:])
        dkv_ref[:, KV:] = dkv_s[:, KV:].astype(BF)


def attend_by(me, qkv, by, out, lse, cos, sin, bq=512, bk=512):
    t = qkv.shape[0]
    wide = _fit(bq, 512)
    mine = lambda i, me: (i, 0)
    still = lambda i, me: (0, 0)
    return call(functools.partial(_attend_by, bq=bq, bk=bk, wide=wide), me, (t // bq,),
                [(qkv, (bq, QW), mine), (qkv, (t, QW), lambda i, me: (0, 1)), (by, (bq, QW), mine), (out, (bq, QW), mine),
                 (lse, (4, bq), lambda i, me: (0, i)), (cos, (t, HALF), still), (sin, (t, HALF), still)],
                [((t, QW), BF, (bq, QW), mine), ((t, QW), BF, (t, QW), still)], 2 * 4 * t * t * 1280 * 5 // 8,
                [pltpu.VMEM((4, HEAD, bq), F32), pltpu.VMEM((t, QW), F32), pltpu.VMEM((bk, wide), jnp.int32)])


def core(t):
    return lax.ppermute(t, "tp", CORE)


def chip(t):
    return lax.ppermute(t, "tp", CHIP)


def after(t, *others):
    return lax.optimization_barrier((t, *others))[0]


def layer(me, x, dy, w):
    n, _ = x.shape
    slot = lambda s: lambda me: me[0] ^ s
    whole = lambda parts: [piece(t, t.shape[0]) for t in parts]
    angle = jnp.arange(4 * n, dtype=F32)[:, None] * THETA ** (-jnp.arange(HALF, dtype=F32) / HALF)
    cos, sin = jnp.cos(angle), jnp.sin(angle)

    a0 = norm(me, x)
    a1 = [core(t) for t in a0]
    a2 = [chip(t) for t in a0]
    dy1 = core(dy)
    act_in = qkv(me, [*a0, *a1], (0, 1), w, cos, sin)
    by_hid_here, = terms(me, [(whole([after(dy, act_in), dy1]), w["w_down"])], nt, KV, joined=True)
    a2 = [after(t, by_hid_here) for t in a2]
    a3 = [core(t) for t in a2]
    dy2 = chip(after(dy, *a2))
    act_in = qkv(me, [*a2, *a3], (2, 3), w, cos, sin, (act_in,))
    heads = lambda s, *deps: piece(after(out, *deps) if deps else out, n, slot(s))
    p3, p2, out, lse = attend(me, act_in, w["wo"], (3, 2))
    r = add_halves(me, p2, core(p3))
    got_0 = chip(r[0])
    got_1 = chip(r[1])
    p1, p0, out, lse = attend(me, after(act_in, *r), w["wo"], (1, 0), (out, lse))
    dy2 = after(dy2, p0)
    dy3 = core(dy2)
    c1 = core(p1)
    by_hid_far, = terms(me, [(whole([dy2, dy3]), w["w_down"])], nt, KV, joined=True)
    h, b_0 = join(me, 0, p0, c1, after(got_0, by_hid_far), x)
    b2_0 = chip(b_0)
    b1_0 = core(b_0)
    h, b_1 = join(me, 1, p0, c1, after(got_1, b_0), x, h)
    b2_1 = chip(b_1)
    b0, b1, b2 = [b_0, b_1], [b1_0, core(b_1)], [b2_0, b2_1]
    units = hidden(me, [*b0, *b1], w["w_gate"], w["w_up"], by_hid_here, KV, 0)
    b2 = [after(t, units[0]) for t in b2]
    b3 = [core(t) for t in b2]
    hid, dg, du = hidden(me, [*b2, *b3], w["w_gate"], w["w_up"], by_hid_far, KV, 1, units)

    def by_b(first, *deps):
        places = lambda t: [piece(t, n, lambda me: first), piece(t, n, lambda me: first - 1)]
        return terms(me, [(places(after(dg, *deps) if deps else dg), w["w_gate"]), (places(du), w["w_up"])], nt, KV)

    q3, q2 = by_b(3)
    q1, q0 = by_b(1, q2)
    r = add(me, after(q2, q0), core(q3))
    dys = whole([dy, dy1, dy2, dy3])
    bs = lambda *deps: whole([after(b0[0], *deps), b0[1], *b1, *b2, *b3])
    dgs, dus = [piece(dg, 4 * n)], [piece(du, 4 * n)]
    got = chip(r)
    by_down = outer(me, [piece(after(hid, r), 4 * n)], dys, TILE, WIDE)
    by_up = outer(me, bs(by_down), dus, TILE, WIDE, (0, 1))
    dh = unjoin(me, q0, core(q1), after(got, by_up), h, dy)
    g2 = chip(dh)
    g1 = core(dh)
    by_gate = outer(me, bs(dh), dgs, TILE, WIDE)
    by_up = outer(me, bs(by_gate), dus, TILE, WIDE, (1, 2), by_up)
    g2 = after(g2, by_up)
    g = [dh, g1, g2, core(g2)]
    by_out = heads_by(me, g, w["wo"], KV)
    dq, dkv = attend_by(me, act_in, by_out, out, lse, cos, sin)

    def by_a(first, *deps):
        places = lambda t, col=0, k=None: [piece(t, n, slot(first), col, k), piece(t, n, slot(first - 1), col, k)]
        return terms(me, [(places(after(dq, *deps) if deps else dq), w["wq"]), (places(dkv, 0, KV), w["wk"]), (places(dkv, 1, KV), w["wv"])], nt, KV)

    s3, s2 = by_a(3)
    s1, s0 = by_a(1, s2)
    r = add(me, after(s2, s0), core(s3))
    got = chip(r)
    by_wo = outer(me, [heads(0, r), heads(1), heads(2), heads(3)], whole(g), QW, KV)
    by_wq, by_wk, by_wv = outer_qkv(me, whole([after(a0[0], by_wo), a0[1], *a1, *a2, *a3]), dq, dkv, range(4), TILE)
    by_up = outer(me, bs(by_wq), dus, TILE, WIDE, (2, 4), by_up)
    r = got
    dx = unjoin(me, s0, core(s1), after(r, by_up), x, dh)
    return dx, by_wq, by_wk, by_wv, by_wo, by_gate, by_up, by_down


NAMES = ("wq", "wk", "wv", "wo", "w_gate", "w_up", "w_down")


def solution(mesh):
    def step(x, dy, *weights):
        me = lax.axis_index("tp").astype(jnp.int32)[None]
        dx, *by_w = layer(me, x[0], dy[0], dict(zip(NAMES, weights, strict=True)))
        return (dx[None], *by_w)

    states, by_columns, by_rows = P("dp", "tp", None), P(None, "tp"), P("tp", None)
    weights = (by_columns, by_columns, by_columns, by_rows, by_columns, by_columns, by_rows)
    own = tuple(P("dp", "tp") if spec == by_columns else P(("dp", "tp"), None) for spec in weights)
    step = jax.shard_map(step, mesh=mesh, in_specs=(states, states, *weights), out_specs=(states, *own), check_vma=False)
    return step
```

```python
import functools

import jax
import jax.numpy as jnp
from jax import lax
from jax.experimental import pallas as pl
from jax.experimental.pallas import tpu as pltpu
from jax.sharding import PartitionSpec as P


LOG2E = 1.4426950408889634
NEG = -1e30
HIDDEN = 2 * NEG
VMEM = 60 * 2**20
HEAD = 256
HALF = HEAD // 2
QW, KV = 1024, 512
TILE, WIDE = 896, 1792
THETA = 10000
CORE = [(0, 1), (1, 0), (2, 3), (3, 2)]
CHIP = [(0, 2), (2, 0), (1, 3), (3, 1)]
BF = jnp.bfloat16
F32 = jnp.float32


def _fit(size, want, unit=128):
    return max(n for n in range(unit, max(min(want, size), unit) + 1, unit) if size % n == 0)


def nn(a, b):
    return lax.dot_general(a, b, (((1,), (0,)), ((), ())), preferred_element_type=F32)


def nt(a, b):
    return lax.dot_general(a, b, (((1,), (1,)), ((), ())), preferred_element_type=F32)


def tn(a, b):
    return lax.dot_general(a, b, (((0,), (0,)), ((), ())), preferred_element_type=F32)


def rows(refs):
    got = [r[:] for r in refs]
    return got[0] if len(got) == 1 else jnp.concatenate(got, axis=0)


def hbm(array):
    return array, None, None


def call(body, me, grid, ins, outs, flops, scratch=(), aliases=None, vmem=VMEM):
    specs = [pl.BlockSpec(memory_space=pl.ANY) if block is None else pl.BlockSpec(block, at, **dict.fromkeys(["pipeline_mode"] * len(more), pl.Buffered(1)))
             for _, block, at, *more in ins]
    arrays = [a for a, *_ in ins]
    moved = sum(a.size * a.dtype.itemsize for a in arrays)
    got = pl.pallas_call(
        body,
        grid_spec=pltpu.PrefetchScalarGridSpec(
            num_scalar_prefetch=1, grid=grid, in_specs=specs,
            out_specs=[pl.BlockSpec(block, at) for _, _, block, at in outs], scratch_shapes=list(scratch)),
        out_shape=[jax.ShapeDtypeStruct(shape, dtype) for shape, dtype, _, _ in outs],
        input_output_aliases={} if aliases is None else aliases,
        compiler_params=pltpu.CompilerParams(dimension_semantics=("arbitrary",) * len(grid), vmem_limit_bytes=vmem),
        cost_estimate=pl.CostEstimate(flops=int(flops), bytes_accessed=moved, transcendentals=0),
    )(me, *arrays)
    return got


ROWS = 24 * 2**20
STEP = 96
STRIP = 16


def strips(work, *refs):
    for at in range(0, STEP, STRIP):
        work(*(ref.at[at : at + STRIP] for ref in refs))


def wide(ref):
    return ref[:].astype(F32)


def by_rows(shift=0):
    return lambda i, me: (i + shift, 0)


def row_kernel(body, me, ins, outs, steps, vmem=VMEM, into=None):
    d = ins[0][0].shape[1]
    specs = [(a, (STEP, d), by_rows(first)) for a, first in ins]
    aliases = {}
    if into is not None:
        aliases = {1 + len(specs): 0}
        specs.append(hbm(into))
    return call(body, me, (steps,), specs, [((n, d), BF, (STEP, d), by_rows(first)) for n, first in outs], 9 * steps * STEP * d, aliases=aliases, vmem=vmem)


def _normed(wide):
    return (wide * lax.rsqrt(jnp.mean(wide * wide, -1, keepdims=True) + 1e-6)).astype(BF)


def _norm(me, x_ref, *a_refs, per):
    for n, ref in enumerate(a_refs):
        @pl.when(pl.program_id(0) // per == n)
        def _():
            ref[:] = _normed(wide(x_ref))


def _halves(body, me, ins, d):
    n = ins[0].shape[0]
    per = n // 2 // STEP
    outs = [((n // 2, d), BF, (STEP, d), lambda i, me: (jnp.minimum(i, per - 1), 0)), ((n // 2, d), BF, (STEP, d), lambda i, me: (jnp.maximum(i - per, 0), 0))]
    return call(functools.partial(body, per=per), me, (2 * per,), [(t, (STEP, d), by_rows()) for t in ins], outs, 4 * n * d, vmem=ROWS)


def norm(me, x):
    return _halves(_norm, me, [x], x.shape[1])


def _add(me, a_ref, b_ref, *o_refs, per):
    for n, ref in enumerate(o_refs):
        @pl.when(pl.program_id(0) // per == n)
        def _():
            ref[:] = (wide(a_ref) + wide(b_ref)).astype(BF)


def add(me, a, b):
    n = a.shape[0]
    return row_kernel(functools.partial(_add, per=n), me, [(a, 0), (b, 0)], [(n, 0)], n // STEP)[0]


def add_halves(me, a, b):
    return _halves(_add, me, [a, b], a.shape[1])


def _join(me, p_ref, c_ref, r_ref, x_ref, *refs):
    def work(p, c, r, x, h_ref, b_ref):
        h = (wide(x) + (wide(p) + wide(c) + wide(r)).astype(BF).astype(F32)).astype(BF)
        h_ref[:] = h
        b_ref[:] = _normed(h.astype(F32))

    strips(work, p_ref, c_ref, r_ref, x_ref, *refs[-2:])


def join(me, half, p, c, r, x, into=None):
    n = x.shape[0]
    per = n // 2 // STEP
    return row_kernel(_join, me, [(p, half * per), (c, half * per), (r, 0), (x, half * per)], [(n, half * per), (n // 2, 0)], per, into=into)


def _unjoin(me, *refs):
    def work(p, c, r, h_ref, g, o_ref):
        by = (wide(p) + wide(c) + wide(r)).astype(BF).astype(F32)
        h = wide(h_ref)
        scale = lax.rsqrt(jnp.mean(h * h, -1, keepdims=True) + 1e-6)
        mix = jnp.sum(by * h, -1, keepdims=True) * (scale * scale * scale / h.shape[1])
        o_ref[:] = (wide(g) + (by * scale - h * mix).astype(BF).astype(F32)).astype(BF)

    strips(work, *refs)


def unjoin(me, p, c, r, h, g):
    n = h.shape[0]
    return row_kernel(_unjoin, me, [(t, 0) for t in (p, c, r, h, g)], [(n, 0)], n // STEP)[0]


def turn(t, cos, sin):
    got = []
    for at in range(0, t.shape[1], HEAD):
        a, b = t[:, at : at + HALF], t[:, at + HALF : at + HEAD]
        got += [a * cos - b * sin, b * cos + a * sin]
    return jnp.concatenate(got, axis=1).astype(BF)


CHUNKS = 2


def copy(src, dst, sem):
    return pltpu.make_async_copy(src, dst, sem)


def _matmul(me, *refs, chunks, left, right, sides, pairs, form, steps, block, source, put, outs):
    refs = list(refs)

    def take(count):
        got, refs[:] = refs[:count], refs[count:]
        return got

    a_refs = [take(len(pieces)) for pieces in left]
    w_refs, x_refs = take(len(right)), take(len(sides))
    refs[:] = refs[len(refs) - outs - 2 * len(left) - 3 * len(source) - 2 * len(sides) :]
    o_refs = take(outs)
    a_s, a_sem, w_s, w_sem, first_sem, x_s, x_sem = take(len(left)), take(len(left)), take(len(source)), take(len(source)), take(len(source)), take(len(sides)), take(len(sides))
    j = pl.program_id(0)
    slot = lax.rem(j, 2)

    def part(c, size):
        return pl.ds(c * (size // chunks), size // chunks)

    def a_copies(c):
        for pieces, ins, dst, sems in zip(left, a_refs, a_s, a_sem):
            at = 0
            for p, ((size, where, col, k), ref) in enumerate(zip(pieces, ins)):
                first = where(me) * size
                cols = pl.ds(col * k + c * (k // chunks), k // chunks)
                yield copy(ref.at[pl.ds(pl.multiple_of(first, size), size), cols], dst.at[pl.ds(at, size), part(c, k)], sems.at[p, c])
                at += size

    def w_first(c):
        for pick, dst, sems in zip(source, w_s, first_sem):
            ref, at = pick(w_refs, 0)
            k = dst.shape[1 if form is nn else 2]
            src = ref.at[part(c, k), pl.ds(at, block)] if form is nn else ref.at[pl.ds(at, block), part(c, k)]
            yield copy(src, dst.at[0, part(c, k), :] if form is nn else dst.at[0, :, part(c, k)], sems.at[c])

    def w_copies(step, at_slot):
        for pick, dst, sems in zip(source, w_s, w_sem):
            ref, at = pick(w_refs, step)
            yield copy(ref.at[:, pl.ds(at, block)] if form is nn else ref.at[pl.ds(at, block), :], dst.at[at_slot], sems.at[at_slot])

    def x_copies(step, at_slot):
        for (per_step, where), ref, dst, sem in zip(sides, x_refs, x_s, x_sem):
            if per_step:
                yield copy(ref.at[:, pl.ds(step * block, block)], dst.at[at_slot], sem.at[at_slot])
            elif isinstance(step, int) and step == 0:
                yield copy(ref.at[pl.ds(where(me), dst.shape[0]), :], dst, sem)

    def begin(step, at_slot):
        for each in (*w_copies(step, at_slot), *x_copies(step, at_slot)):
            each.start()

    def ahead():
        if isinstance(source[0](w_refs, 0)[1], int) and len(right) > len(source):
            for step in range(2, steps):
                pl.when(j == step - 1)(functools.partial(begin, step, step % 2))
        else:
            pl.when(j + 1 < steps)(lambda: begin(j + 1, 1 - slot))

    def finish(totals, at_slot):
        put(me, j, totals, [x.at[at_slot] if side[0] else x for side, x in zip(sides, x_s)], o_refs)

    @pl.when(j == 0)
    def _():
        for c in range(chunks):
            for each in (*a_copies(c), *w_first(c)):
                each.start()
        for each in x_copies(0, 0):
            each.start()
        if steps > 1:
            begin(1, 1)
        totals = {}
        for c in range(chunks):
            for each in (*a_copies(c), *w_first(c)):
                each.wait()
            for l, r, t in pairs:
                k = a_s[l].shape[1]
                w = w_s[r][0, part(c, k), :] if form is nn else w_s[r][0, :, part(c, k)]
                got = form(a_s[l][:, part(c, k)], w)
                totals[t] = totals[t] + got if t in totals else got
        for each in x_copies(0, 0):
            each.wait()
        finish(totals, 0)

    @pl.when(j > 0)
    def _():
        ahead()
        for each in (*w_copies(1, slot), *x_copies(1, slot)):
            each.wait()
        totals = {}
        for l, r, t in pairs:
            got = form(a_s[l][:], w_s[r][slot])
            totals[t] = totals[t] + got if t in totals else got
        finish(totals, slot)


by_step = lambda r, block: lambda refs, step: (refs[r], step * block)


def matmul(me, left, right, pairs, form, block, steps, put, outs, sides=(), source=None, into=(), chunks=CHUNKS):
    rows_of = [sum(p[1] for p in pieces) for pieces in left]
    source = [by_step(r, block) for r in range(len(right))] if source is None else source
    ks = [right[r].shape[form is nt] for r in range(len(source))]
    ins = [(p[0], None, None) for pieces in left for p in pieces] + [(w, None, None) for w in right] + [(x[0], None, None) for x in sides]
    aliases = {1 + len(ins) + i: i for i in range(len(into))}
    ins += [(t, None, None) for t in into]
    dma = pltpu.SemaphoreType.DMA
    scratch = [pltpu.VMEM((m, pieces[0][4]), BF) for m, pieces in zip(rows_of, left)] + [dma((len(pieces), chunks)) for pieces in left]
    scratch += [pltpu.VMEM((2, k, block) if form is nn else (2, block, k), BF) for k in ks] + [dma((2,)) for _ in ks] + [dma((chunks,)) for _ in ks]
    scratch += [pltpu.VMEM((2, x[0].shape[0], block) if x[1] else (x[2][1], x[0].shape[1]), x[0].dtype) for x in sides] + [dma((2,)) if x[1] else dma for x in sides]
    body = functools.partial(_matmul, chunks=chunks, left=[[(p[1], p[2], p[3], p[4]) for p in pieces] for pieces in left], right=right, pairs=pairs, form=form, steps=steps,
                             sides=[(x[1], None if x[1] else x[2][0]) for x in sides], block=block, source=source, put=put, outs=len(outs))
    flops = 2 * steps * block * sum(rows_of[l] * ks[r] for l, r, _ in pairs)
    return call(body, me, (steps,), ins, outs, flops, scratch, aliases)


def _put_qkv(me, j, totals, sides, o_refs, *, half, tops):
    got = totals[0].astype(BF)
    cos_ref, sin_ref = sides
    for i, top in enumerate(tops):
        at = pl.multiple_of(top(me), half)
        part = got[i * half : (i + 1) * half]
        turned = turn(part.astype(F32), cos_ref[pl.ds(at, half), :], sin_ref[pl.ds(at, half), :])
        o_refs[0][pl.ds(at, half), :] = jnp.where(j < 3, turned, part)


def qkv(me, parts, slots, w, cos, sin, into=()):
    half = sum(a.shape[0] for a in parts) // 2
    chip = lambda me: (me[0] ^ slots[0]) // 2
    tops = [functools.partial(lambda me, s: (me[0] ^ s) % 2 * half, s=s) for s in slots]
    pick = lambda refs, step: (refs[max(step - 1, 0)], 512 if step == 1 else 0)
    side = lambda t: (t, False, (lambda me: pl.multiple_of(chip(me) * 2 * half, 2 * half), 2 * half))
    return matmul(me, [[piece(a, a.shape[0]) for a in parts]], [w["wq"], w["wk"], w["wv"]], [(0, 0, 0)], nn, KV, 4,
                  functools.partial(_put_qkv, half=half, tops=tops), [((4 * half, 2048), BF, (2 * half, KV), lambda j, me: (chip(me), j))],
                  [side(cos), side(sin)], [pick], into)[0]


def _put_terms(me, j, totals, sides, o_refs):
    total, at = totals[0].astype(BF), 0
    for o_ref in o_refs:
        o_ref[:] = total[at : at + o_ref.shape[0]]
        at += o_ref.shape[0]


def terms(me, pairs, form, block, joined=False, chunks=CHUNKS):
    cols = pairs[0][1].shape[form is nn]
    sizes = [p[1] for p in pairs[0][0]]
    outs = [((size, cols), BF, (size, block), lambda j, me: (0, j)) for size in ([sum(sizes)] if joined else sizes)]
    return matmul(me, [p[0] for p in pairs], [p[1] for p in pairs], [(i, i, 0) for i in range(len(pairs))], form, block, cols // block, _put_terms, outs, chunks=chunks)


def _put_hidden(me, j, totals, sides, o_refs):
    gate, up, by = totals[0], totals[1], sides[0][:].astype(F32)
    sig = 1 / (1 + jnp.exp(-gate))
    silu = gate * sig
    hid_ref, dg_ref, du_ref = o_refs
    hid_ref[:] = (silu * up).astype(BF)
    du_ref[:] = (by * silu).astype(BF)
    dg_ref[:] = (by * up * (sig * (1 + gate * (1 - sig)))).astype(BF)


def hidden(me, parts, w_gate, w_up, by, block, place, into=()):
    f, m = w_gate.shape[1], by.shape[0]
    outs = [((2 * m, f), BF, (m, block), lambda j, me: (place, j))] * 3
    return matmul(me, [[piece(p, p.shape[0]) for p in parts]], [w_gate, w_up], [(0, 0, 0), (0, 1, 1)], nn, block,
                  f // block, _put_hidden, outs, [(by, True, None)], None, into)


def _outer(me, *refs, na, nb):
    refs[-1][:] = tn(rows(refs[:na]), rows(refs[na : na + nb])).astype(BF)


def piece(array, size, where=None, col=0, k=None):
    return (array, size, (lambda me: 0) if where is None else where, col, array.shape[1] if k is None else k)


def outer(me, left, right, bm, bn, span=None, into=None):
    ins, tokens = [], sum(p[1] for p in left)
    m, n = left[0][4], right[0][4]
    first, last = (0, m // bm) if span is None else span
    for pieces, block, axis in ((left, bm, 0), (right, bn, 1)):
        for array, size, where, col, k in pieces:
            at = functools.partial(lambda i, j, me, where, axis, shift: (where(me), (i, j)[axis] + shift), where=where, axis=axis,
                                   shift=col * (k // block) + first * (1 - axis))
            ins.append((array, (size, block), at))
    if into is not None:
        ins.append(hbm(into))
    return call(functools.partial(_outer, na=len(left), nb=len(right)), me, (last - first, n // bn), ins,
                [((m, n), BF, (bm, bn), lambda i, j, me: (i + first, j))], 2 * tokens * (last - first) * bm * n,
                aliases=None if into is None else {len(ins): 0})[0]


def _outer_qkv(me, *refs, n, m):
    right = jnp.concatenate([rows(refs[n : n + m]), rows(refs[n + m : n + 2 * m])], axis=1)
    got = tn(rows(refs[:n]), right).astype(BF)
    at = 0
    for o_ref in refs[-3:]:
        o_ref[:] = got[:, at : at + o_ref.shape[1]]
        at += o_ref.shape[1]


def outer_qkv(me, left, dq, dkv, slots, bm):
    d, n = left[0][0].shape[1], dq.shape[0] // len(slots)
    ins = [(a, (size, bm), lambda i, me: (0, i)) for a, size, *_ in left]
    ins += [(t, (n, QW), functools.partial(lambda i, me, s: (me[0] ^ s, 0), s=s)) for t in (dq, dkv) for s in slots]
    outs = [((d, width), BF, (bm, width), lambda i, me: (i, 0)) for width in (QW, KV, KV)]
    return call(functools.partial(_outer_qkv, n=len(left), m=len(slots)), me, (d // bm,), ins, outs, 2 * dq.shape[0] * d * 2048)


def _put_heads(me, j, totals, sides, o_refs, *, size):
    got = totals[0].astype(BF)
    for s in range(got.shape[0] // size):
        o_refs[0][pl.ds(pl.multiple_of((me[0] ^ s) * size, size), size), :] = got[s * size : (s + 1) * size]


def heads_by(me, parts, wo, block):
    size = parts[0].shape[0]
    outs = [((4 * size, wo.shape[0]), BF, (4 * size, block), lambda j, me: (0, j))]
    return matmul(me, [[piece(p, size) for p in parts]], [wo], [(0, 0, 0)], nt, block, wo.shape[0] // block,
                  functools.partial(_put_heads, size=size), outs)[0]


def q_cols(h):
    return slice(h * HEAD, h * HEAD + HEAD)


def k_cols(h):
    return q_cols(h // 2)


def v_cols(h):
    return q_cols(h // 2 + 2)


def _gap(bk, wide):
    return lax.broadcasted_iota(jnp.int32, (bk, wide), 1) - lax.broadcasted_iota(jnp.int32, (bk, wide), 0)


def _attend(me, q_ref, kv_ref, wo_ref, *rest, slots, n, wide):
    *p_refs, o_ref, lse_ref, top_s, mix_s, gap_s, wo_s, wo_sem = rest[-7 - len(slots) :]
    i = pl.program_id(0)
    wo_copy = copy(wo_ref, wo_s, wo_sem)
    mine = me[0] ^ (slots[0] - i)
    scale = HEAD**-0.5
    e = scale * LOG2E
    heads = q_ref.shape[1] // HEAD
    pieces = [(h, at) for h in range(heads) for at in range(0, n, wide)]

    @pl.when(i == 0)
    def _():
        wo_copy.start()
        gap_s[:] = _gap(n, wide)

    top_s[:] = jnp.full_like(top_s, NEG)
    mix_s[:] = jnp.zeros_like(mix_s)
    ones = jnp.ones((8, n), BF)

    def block(j, masked):
        here = pl.ds(pl.multiple_of(j * n, n), n)
        scores = [nt(kv_ref[here, k_cols(h)], q_ref[at : at + wide, q_cols(h)]) for h, at in pieces]
        weights, keeps = [], []
        for (h, at), s in zip(pieces, scores):
            if masked:
                s = jnp.where(gap_s[:] >= -at, s, HIDDEN)
            old = top_s[h : h + 1, at : at + wide]
            top = jnp.maximum(old, s.max(axis=0, keepdims=True))
            top_s[h : h + 1, at : at + wide] = top
            weights.append(jnp.exp2((s - top) * e).astype(BF))
            keeps.append(jnp.exp2((old - top) * e))
        for (h, at), p, keep in zip(pieces, weights, keeps):
            v = kv_ref[here, v_cols(h)]
            values = jnp.concatenate([v.T, ones], axis=0)
            mix_s[h, :, at : at + wide] = mix_s[h, :, at : at + wide] * keep + nn(values, p)

    lax.fori_loop(0, mine, lambda j, _: block(j, False), None)
    block(mine, True)
    for h in range(heads):
        top, total = top_s[h : h + 1, :], mix_s[h, HEAD : HEAD + 1, :]
        o_ref[:, q_cols(h)] = (mix_s[h, :HEAD, :] * (1 / total)).T.astype(BF)
        lse_ref[h : h + 1, :] = top * scale + jnp.log(total)
    pl.when(i == 0)(wo_copy.wait)
    for k, p_ref in enumerate(p_refs):
        @pl.when(i == k)
        def _():
            for at in range(0, p_ref.shape[1], 896):
                p_ref[:, at : at + 896] = nn(o_ref[:], wo_s[:, at : at + 896]).astype(BF)


def attend(me, qkv, wo, slots, into=()):
    t, d = qkv.shape[0], wo.shape[1]
    n = t // 4
    wide = _fit(n, KV)
    mine = lambda i, me: me[0] ^ (slots[0] - i)
    ins = [(qkv, (n, QW), lambda i, me: (mine(i, me), 0)), (qkv, (t, QW), lambda i, me: (0, 1), 1), hbm(wo)]
    aliases = {1 + len(ins) + i: len(slots) + i for i in range(len(into))}
    ins += [(a, None, None) for a in into]
    outs = [((n, d), BF, (n, d), lambda i, me: (0, 0))] * len(slots)
    outs += [((t, QW), BF, (n, QW), lambda i, me: (mine(i, me), 0)), ((4, t), F32, (4, n), lambda i, me: (0, mine(i, me)))]
    return call(functools.partial(_attend, slots=slots, n=n, wide=wide), me, (len(slots),), ins, outs, 2 * 2 * n * (4 * 512 * t // 2 + QW * d),
                [pltpu.VMEM((8, n), F32), pltpu.VMEM((4, HEAD + 8, n), F32), pltpu.VMEM((n, wide), jnp.int32),
                 pltpu.VMEM(wo.shape, BF), pltpu.SemaphoreType.DMA], aliases)


def _attend_by(me, q_ref, kv_ref, do_ref, o_ref, lse_ref, cos_ref, sin_ref, dq_ref, dkv_ref, dq_s, dkv_s, gap_s, *, bq, bk, wide):
    iq = pl.program_id(0)
    scale = HEAD**-0.5
    e = scale * LOG2E
    heads = q_ref.shape[1] // HEAD
    pieces = [(h, at) for h in range(heads) for at in range(0, bq, wide)]

    @pl.when(iq == 0)
    def _():
        gap_s[:] = _gap(bk, wide)
        dkv_s[:] = jnp.zeros_like(dkv_s)

    dq_s[:] = jnp.zeros_like(dq_s)
    lses = [lse_ref[h : h + 1, at : at + wide] * LOG2E for h, at in pieces]
    deltas = []
    for h, at in pieces:
        own = (slice(at, at + wide), q_cols(h))
        deltas.append((do_ref[own].astype(F32) * o_ref[own].astype(F32)).T.sum(axis=0, keepdims=True))

    def block(j, masked):
        here = pl.ds(pl.multiple_of(j * bk, bk), bk)
        k_of = lambda h: kv_ref[here, k_cols(h)]
        v_of = lambda h: kv_ref[here, v_cols(h)]
        qs = [q_ref[at : at + wide, q_cols(h)] for h, at in pieces]
        dos = [do_ref[at : at + wide, q_cols(h)] for h, at in pieces]
        scores = [nt(k_of(h), x) for (h, _), x in zip(pieces, qs)]
        dps = [nt(v_of(h), x) for (h, _), x in zip(pieces, dos)]
        for n, (h, at) in enumerate(pieces):
            p = jnp.exp2(scores[n] * e - lses[n])
            if masked:
                p = jnp.where(gap_s[:] >= j * bk - iq * bq - at, p, 0.0)
            ds = (p * (dps[n] - deltas[n])).astype(BF)
            dkv_s[here, v_cols(h)] += nn(p.astype(BF), dos[n])
            dkv_s[here, k_cols(h)] += nn(ds, qs[n])
            dq_s[h, :, at : at + wide] += nn(k_of(h).T, ds)

    lax.fori_loop(0, iq * bq // bk, lambda j, _: block(j, False), None)
    lax.fori_loop(iq * bq // bk, ((iq + 1) * bq + bk - 1) // bk, lambda j, _: block(j, True), None)
    mine = pl.ds(pl.multiple_of(iq * bq, bq), bq)
    cos, sin = cos_ref[mine, :], sin_ref[mine, :]
    for h in range(heads):
        dq = (dq_s[h] * scale).T.astype(BF).astype(F32)
        dq_ref[:, q_cols(h)] = turn(dq, cos, -sin)

    @pl.when(iq == pl.num_programs(0) - 1)
    def _():
        dk = (dkv_s[:, :KV] * scale).astype(BF).astype(F32)
        dkv_ref[:, :KV] = turn(dk, cos_ref[:], -sin_ref[:])
        dkv_ref[:, KV:] = dkv_s[:, KV:].astype(BF)


def attend_by(me, qkv, by, out, lse, cos, sin, bq=512, bk=512):
    t = qkv.shape[0]
    wide = _fit(bq, 512)
    mine = lambda i, me: (i, 0)
    still = lambda i, me: (0, 0)
    return call(functools.partial(_attend_by, bq=bq, bk=bk, wide=wide), me, (t // bq,),
                [(qkv, (bq, QW), mine), (qkv, (t, QW), lambda i, me: (0, 1)), (by, (bq, QW), mine), (out, (bq, QW), mine),
                 (lse, (4, bq), lambda i, me: (0, i)), (cos, (t, HALF), still), (sin, (t, HALF), still)],
                [((t, QW), BF, (bq, QW), mine), ((t, QW), BF, (t, QW), still)], 2 * 4 * t * t * 1280 * 5 // 8,
                [pltpu.VMEM((4, HEAD, bq), F32), pltpu.VMEM((t, QW), F32), pltpu.VMEM((bk, wide), jnp.int32)])


def core(t):
    return lax.ppermute(t, "tp", CORE)


def chip(t):
    return lax.ppermute(t, "tp", CHIP)


def after(t, *others):
    return lax.optimization_barrier((t, *others))[0]


def layer(me, x, dy, w):
    n, _ = x.shape
    slot = lambda s: lambda me: me[0] ^ s
    whole = lambda parts: [piece(t, t.shape[0]) for t in parts]
    angle = jnp.arange(4 * n, dtype=F32)[:, None] * THETA ** (-jnp.arange(HALF, dtype=F32) / HALF)
    cos, sin = jnp.cos(angle), jnp.sin(angle)

    a0 = norm(me, x)
    a1 = [core(t) for t in a0]
    a2 = [chip(t) for t in a0]
    dy1 = core(dy)
    act_in = qkv(me, [*a0, *a1], (0, 1), w, cos, sin)
    by_hid_here, = terms(me, [(whole([after(dy, act_in), dy1]), w["w_down"])], nt, KV, joined=True)
    a2 = [after(t, by_hid_here) for t in a2]
    a3 = [core(t) for t in a2]
    dy2 = chip(after(dy, *a2))
    act_in = qkv(me, [*a2, *a3], (2, 3), w, cos, sin, (act_in,))
    heads = lambda s, *deps: piece(after(out, *deps) if deps else out, n, slot(s))
    p3, p2, out, lse = attend(me, act_in, w["wo"], (3, 2))
    r = add_halves(me, p2, core(p3))
    got_0 = chip(r[0])
    got_1 = chip(r[1])
    p1, p0, out, lse = attend(me, after(act_in, *r), w["wo"], (1, 0), (out, lse))
    dy2 = after(dy2, p0)
    dy3 = core(dy2)
    c1 = core(p1)
    by_hid_far, = terms(me, [(whole([dy2, dy3]), w["w_down"])], nt, KV, joined=True)
    h, b_0 = join(me, 0, p0, c1, after(got_0, by_hid_far), x)
    b2_0 = chip(b_0)
    b1_0 = core(b_0)
    h, b_1 = join(me, 1, p0, c1, after(got_1, b_0), x, h)
    b2_1 = chip(b_1)
    b0, b1, b2 = [b_0, b_1], [b1_0, core(b_1)], [b2_0, b2_1]
    units = hidden(me, [*b0, *b1], w["w_gate"], w["w_up"], by_hid_here, KV, 0)
    b2 = [after(t, units[0]) for t in b2]
    b3 = [core(t) for t in b2]
    hid, dg, du = hidden(me, [*b2, *b3], w["w_gate"], w["w_up"], by_hid_far, KV, 1, units)

    def by_b(first, *deps):
        places = lambda t: [piece(t, n, lambda me: first), piece(t, n, lambda me: first - 1)]
        return terms(me, [(places(after(dg, *deps) if deps else dg), w["w_gate"]), (places(du), w["w_up"])], nt, KV)

    q3, q2 = by_b(3)
    q1, q0 = by_b(1, q2)
    r = add(me, after(q2, q0), core(q3))
    dys = whole([dy, dy1, dy2, dy3])
    bs = lambda *deps: whole([after(b0[0], *deps), b0[1], *b1, *b2, *b3])
    dgs, dus = [piece(dg, 4 * n)], [piece(du, 4 * n)]
    got = chip(r)
    by_down = outer(me, [piece(after(hid, r), 4 * n)], dys, TILE, WIDE)
    by_up = outer(me, bs(by_down), dus, TILE, WIDE, (0, 1))
    dh = unjoin(me, q0, core(q1), after(got, by_up), h, dy)
    g2 = chip(dh)
    g1 = core(dh)
    by_gate = outer(me, bs(dh), dgs, TILE, WIDE)
    by_up = outer(me, bs(by_gate), dus, TILE, WIDE, (1, 2), by_up)
    g2 = after(g2, by_up)
    g = [dh, g1, g2, core(g2)]
    by_out = heads_by(me, g, w["wo"], KV)
    dq, dkv = attend_by(me, act_in, by_out, out, lse, cos, sin)

    def by_a(first, *deps):
        places = lambda t, col=0, k=None: [piece(t, n, slot(first), col, k), piece(t, n, slot(first - 1), col, k)]
        return terms(me, [(places(after(dq, *deps) if deps else dq), w["wq"]), (places(dkv, 0, KV), w["wk"]), (places(dkv, 1, KV), w["wv"])], nt, KV)

    s3, s2 = by_a(3)
    s1, s0 = by_a(1, s2)
    r = add(me, after(s2, s0), core(s3))
    got = chip(r)
    by_wo = outer(me, [heads(0, r), heads(1), heads(2), heads(3)], whole(g), QW, KV)
    by_wq, by_wk, by_wv = outer_qkv(me, whole([after(a0[0], by_wo), a0[1], *a1, *a2, *a3]), dq, dkv, range(4), TILE)
    by_up = outer(me, bs(by_wq), dus, TILE, WIDE, (2, 4), by_up)
    r = got
    dx = unjoin(me, s0, core(s1), after(r, by_up), x, dh)
    return dx, by_wq, by_wk, by_wv, by_wo, by_gate, by_up, by_down


NAMES = ("wq", "wk", "wv", "wo", "w_gate", "w_up", "w_down")


def solution(mesh):
    def step(x, dy, *weights):
        me = lax.axis_index("tp").astype(jnp.int32)[None]
        dx, *by_w = layer(me, x[0], dy[0], dict(zip(NAMES, weights, strict=True)))
        return (dx[None], *by_w)

    states, by_columns, by_rows = P("dp", "tp", None), P(None, "tp"), P("tp", None)
    weights = (by_columns, by_columns, by_columns, by_rows, by_columns, by_columns, by_rows)
    own = tuple(P("dp", "tp") if spec == by_columns else P(("dp", "tp"), None) for spec in weights)
    step = jax.shard_map(step, mesh=mesh, in_specs=(states, states, *weights), out_specs=(states, *own), check_vma=False)
    return step
```
